128 devices in a mesh: rep: 32 (over x, y_hi, z), tp: 4 (over y_lo, core).
Axes of the slice: x: 4, y: 4 (y_hi: 2, y_lo: 2; y = y_hi * 2 + y_lo), z: 4, core: 2. Of those that a mesh axis runs over, the one named last changes fastest.
Arguments:
- q_weight: float32 [5120, 5120], P(('rep', 'tp')), may hold values from -0.078125 to 0.078125
- key_projection_weight: float32 [1024, 5120], P(('rep', 'tp')), may hold values from -0.078125 to 0.078125
- value_projection_weight: float32 [1024, 5120], P(('rep', 'tp')), may hold values from -0.078125 to 0.078125
- tokens: bfloat16 [32768, 5120], P(('rep', 'tp')), may hold values from -6 to 6
Outputs:
- combined_query_key_value: bfloat16 [7168, 5120], P('tp')
- projected: bfloat16 [32768, 7168], P('rep', 'tp')
The draws below stay inside these ranges and needn't reach their ends.
All inputs are finite; a program needn't handle non-finite values.
Results may differ from the reference program's by a relative error of at most 0.0049.
Values may be sent and summed in bfloat16 or wider, within the bound.
A program may use at most 192 MiB of HBM per device.

```python
import jax
import jax.numpy as jnp

MODEL_WIDTH = 5120
HQ = 40
KEY_VALUE_HEADS = 8
HEAD_SIZE = 128
TOKENS = 32768
N_TP = 4


def block_scale(key, shape, cuts, smallest, top_value):
    level, own = 1.0, jax.random.fold_in(key, 6)
    for dim, shards_of in cuts:
        heights = jnp.exp(jax.random.uniform(jax.random.fold_in(own, dim), (shards_of,), jnp.float32, smallest / len(cuts), top_value / len(cuts)))
        level = level * jnp.repeat(heights, shape[dim] // shards_of).reshape([-1 if axis == dim else 1 for axis in range(len(shape))])
    return level


def bell_draw(key, dims, width, bound, shards=(), kind=jnp.bfloat16):
    array = width * jax.random.normal(key, dims, jnp.float32)
    if shards:
        array = array * block_scale(key, dims, shards, -0.22, 0.18)
    return jnp.clip(array, -bound, bound).astype(kind)


def setup_inputs(seed: int = 0) -> dict:
    seeds = jax.random.split(jax.random.key(seed), 5)
    return {
        "q_weight": bell_draw(seeds[0], (HQ * HEAD_SIZE, MODEL_WIDTH), MODEL_WIDTH ** -0.5, 0.078125, ((0, 128),), jnp.float32),
        "key_projection_weight": bell_draw(seeds[1], (KEY_VALUE_HEADS * HEAD_SIZE, MODEL_WIDTH), MODEL_WIDTH ** -0.5, 0.078125, ((0, 128),), jnp.float32),
        "value_projection_weight": bell_draw(seeds[2], (KEY_VALUE_HEADS * HEAD_SIZE, MODEL_WIDTH), MODEL_WIDTH ** -0.5, 0.078125, ((0, 128),), jnp.float32),
        "tokens": bell_draw(seeds[3], (TOKENS, MODEL_WIDTH), 1.0, 6.0, ((0, 128),)),
    }


def reference(q_weight, key_projection_weight, value_projection_weight, tokens):
    blocks = []
    for source in (q_weight, key_projection_weight, value_projection_weight):
        rounded = source.astype(jnp.bfloat16)
        blocks.append(rounded.reshape(N_TP, -1, MODEL_WIDTH))
    combined_query_key_value = jnp.concatenate(blocks, axis=1).reshape(-1, MODEL_WIDTH)
    projected = jnp.dot(tokens, combined_query_key_value.T, preferred_element_type=jnp.float32).astype(jnp.bfloat16)
    return combined_query_key_value, projected
```

```python
import functools

import jax
import jax.numpy as jnp
from jax import lax
from jax.experimental import pallas as pl
from jax.experimental.pallas import tpu as pltpu
from jax.sharding import PartitionSpec as P

MESH = pl.DeviceIdType.MESH
SUB = 8


def gather_kernel(shape, shard, toks, w, t4, wsend, wrecv, psend, tsend, trecv, loc):
    qr, kr = shape
    n = qr + 2 * kr
    qn, kn = 32 * qr, 32 * kr
    rep, tp = lax.axis_index("rep"), lax.axis_index("tp")
    x, yh, z = rep // 8, (rep // 4) % 2, rep % 4
    thi, tlo = tp // 2, tp % 2

    def at(x_, yh_, z_):
        return x_ * 8 + yh_ * 4 + z_

    x1 = x + 1 - 2 * (x % 2)
    x3 = 3 - x
    role0 = x == tp
    role3 = x == 3 - tp

    def pieces(j):
        return tuple(
            pl.ds(pl.multiple_of(a + j * r, SUB), r)
            for a, r in ((0, qr), (qn, kr), (qn + kn, kr))
        )

    shard_pieces = (pl.ds(0, qr), pl.ds(qr, kr), pl.ds(qr + kr, kr))

    def whole(sem):
        return pltpu.make_async_copy(w.at[pl.ds(0, n)], w.at[pl.ds(0, n)], sem)

    def send(src, pairs, dst_sem, src_sem, dev):
        for s, d in pairs:
            pltpu.make_async_remote_copy(
                src_ref=src.at[s], dst_ref=w.at[d], send_sem=src_sem, recv_sem=dst_sem,
                device_id=dev, device_id_type=MESH,
            ).start()

    me = (yh * 4 + z) * 4 + tp
    pairs = list(zip(shard_pieces, pieces(me)))

    @pl.when(role0)
    def _():
        for s, d in pairs:
            pltpu.make_async_copy(shard.at[s], w.at[d], wrecv.at[me]).start()

    @pl.when(jnp.logical_not(role0))
    def _():
        send(shard, pairs, wrecv.at[me], psend.at[0], (rep, x))

    send(shard, pairs, wrecv.at[me], psend.at[1], (at(x, 1 - yh, z), x))

    rows = toks.shape[0]
    half = rows // 2

    def slot_rows(slot, part):
        return pl.ds(pl.multiple_of(slot * rows + part * half, half), half)

    sib = thi * 2 + (1 - tlo)
    far = (1 - thi) * 2 + tlo
    fars = (1 - thi) * 2 + (1 - tlo)
    own = pltpu.make_async_copy(toks, t4.at[pl.ds(pl.multiple_of(tp * rows, rows), rows)], loc)
    own.start()

    def tok(src, slot, part, sem, dev):
        return pltpu.make_async_remote_copy(
            src_ref=src, dst_ref=t4.at[slot_rows(slot, part)],
            send_sem=tsend.at[sem], recv_sem=trecv.at[slot, part],
            device_id=(rep, dev), device_id_type=MESH,
        )

    for part in range(2):
        tok(toks.at[pl.ds(part * half, half)], tp, part, part, far).start()
    for part in range(2):
        tok(toks.at[pl.ds(part * half, half)], tp, part, 2 + part, sib).start()

    def wait_tok(slot, part):
        ref = t4.at[slot_rows(slot, part)]
        pltpu.make_async_copy(ref, ref, trecv.at[slot, part]).wait()

    def relay(part):
        wait_tok(far, part)
        tok(t4.at[slot_rows(far, part)], far, part, 4 + part, sib).start()

    def plan(i, d):
        zs = (z + d) % 4
        h, m, c = i // 4, (i // 2) % 2, i % 2
        tq = ((thi + m + h) % 2) * 2 + (tlo + c) % 2
        j = (((yh + h) % 2) * 4 + zs) * 4 + tq
        odd = jnp.logical_and(c == 1, jnp.logical_or(i < 7, zs % 2 == 1))
        zact = jnp.logical_or(role0, jnp.logical_not(odd))
        xact = odd if d else jnp.bool_(True)
        out = []
        if d in (0, 3):
            c0 = zact if d == 0 else jnp.logical_and(zact, m == 0)
            out.append((0, c0, (at(x, yh, (z + 1) % 4), tp)))
        if d in (0, 1):
            c0 = zact if d == 0 else jnp.logical_and(zact, m == 1)
            out.append((1, c0, (at(x, yh, (z + 3) % 4), tp)))
        out.append((2, jnp.logical_and(jnp.logical_or(role0, role3), xact), (at(x1, yh, z), tp)))
        out.append((3, jnp.logical_and(role0, xact), (at(x3, yh, z), tp)))
        return j, out

    LAG = ((0, 0), (1, 1), (3, 1), (2, 2))

    def step(u, carry):
        for d, lag in LAG:
            i = u - lag

            @pl.when(jnp.logical_and(i >= 0, i < 8))
            def _(i=i, d=d):
                j, out = plan(i, d)
                whole(wrecv.at[j]).wait()
                for s, cond, dev in out:
                    @pl.when(cond)
                    def _(s=s, dev=dev):
                        pr = [(p, p) for p in pieces(j)]
                        send(w, pr, wrecv.at[j], wsend.at[s, i * 4 + d], dev)

        for part, when in ((0, 5), (1, 8)):
            @pl.when(u == when)
            def _(part=part):
                relay(part)
        return carry

    lax.fori_loop(0, 10, step, 0)

    own.wait()
    for slot in (sib, fars):
        for part in range(2):
            wait_tok(slot, part)
    for s in range(6):
        ref = t4.at[pl.ds(0, half)]
        pltpu.make_async_copy(ref, ref, tsend.at[s]).wait()

    @pl.when(jnp.logical_not(role0))
    def _():
        whole(psend.at[0]).wait()

    whole(psend.at[1]).wait()

    def drain(i, carry):
        for d in range(4):
            _, out = plan(i, d)
            for s, cond, _dev in out:
                @pl.when(cond)
                def _(s=s):
                    whole(wsend.at[s, i * 4 + d]).wait()
        return carry

    lax.fori_loop(0, 8, drain, 0)


def product_kernel(w, t, w_out, p_out, acc, wsem, psem):
    keep = pltpu.make_async_copy(w, w_out, wsem)
    keep.start()
    cols = 256

    def step(i, carry):
        at = pl.ds(pl.multiple_of(i * cols, cols), cols)
        acc[:, at] = lax.dot_general(
            t[...], w[at, :], (((1,), (1,)), ((), ())), preferred_element_type=jnp.float32
        ).astype(jnp.bfloat16)
        return carry

    lax.fori_loop(0, w.shape[0] // cols, step, 0)
    done = pltpu.make_async_copy(acc, p_out, psem)
    done.start()
    done.wait()
    keep.wait()


def shards(q_weight, key_projection_weight, value_projection_weight, tokens):
    width = q_weight.shape[1]
    qr, kr = q_weight.shape[0], key_projection_weight.shape[0]
    rows = 32 * (qr + 2 * kr)
    count = 4 * tokens.shape[0]
    shard = jnp.concatenate(
        [q_weight, key_projection_weight, value_projection_weight], 0
    ).astype(jnp.bfloat16)
    w, t = pl.pallas_call(
        functools.partial(gather_kernel, (qr, kr)),
        out_shape=(
            pltpu.VMEM((rows, width), jnp.bfloat16),
            pltpu.VMEM((count, width), jnp.bfloat16),
        ),
        in_specs=[
            pl.BlockSpec(memory_space=pltpu.VMEM),
            pl.BlockSpec(memory_space=pl.ANY),
        ],
        out_specs=(pl.BlockSpec(memory_space=pl.ANY),) * 2,
        scratch_shapes=[
            pltpu.SemaphoreType.DMA((4, 32)),
            pltpu.SemaphoreType.DMA((32,)),
            pltpu.SemaphoreType.DMA((2,)),
            pltpu.SemaphoreType.DMA((6,)),
            pltpu.SemaphoreType.DMA((4, 2)),
            pltpu.SemaphoreType.DMA,
        ],
        compiler_params=pltpu.CompilerParams(
            has_side_effects=True, vmem_limit_bytes=4 << 20
        ),
        name="gather",
    )(shard, pltpu.with_memory_space_constraint(tokens, pltpu.HBM))
    return pl.pallas_call(
        product_kernel,
        out_shape=(
            jax.ShapeDtypeStruct((rows, width), jnp.bfloat16),
            jax.ShapeDtypeStruct((count, rows), jnp.bfloat16),
        ),
        in_specs=[pl.BlockSpec(memory_space=pltpu.VMEM)] * 2,
        out_specs=(pl.BlockSpec(memory_space=pltpu.HBM),) * 2,
        scratch_shapes=[
            pltpu.VMEM((count, rows), jnp.bfloat16),
            pltpu.SemaphoreType.DMA,
            pltpu.SemaphoreType.DMA,
        ],
        compiler_params=pltpu.CompilerParams(vmem_limit_bytes=20 << 20),
        name="product",
    )(
        pltpu.with_memory_space_constraint(w, pltpu.VMEM),
        pltpu.with_memory_space_constraint(t, pltpu.VMEM),
    )


def solution(mesh):
    both = P(("rep", "tp"), None)
    return jax.shard_map(
        shards, mesh=mesh, in_specs=(both,) * 4, out_specs=(P("tp", None), P("rep", "tp")),
        check_vma=False,
    )
```

```python
import functools

import jax
import jax.numpy as jnp
from jax import lax
from jax.experimental import pallas as pl
from jax.experimental.pallas import tpu as pltpu
from jax.sharding import PartitionSpec as P

MESH = pl.DeviceIdType.MESH
SUB = 8
COLS = 128

CLASSES = "BCBABBBc"
HALF = (0, 0, 1, 1, 0, 0, 1, 1)
ORDER = (
    (0, 0), (1, 0), (2, 0), (3, 0), (0, 1), (1, 1), (0, 3), (1, 3),
    (4, 0), (2, 1), (3, 3), (3, 1), (5, 0), (2, 3), (1, 2), (0, 2),
    (3, 2), (2, 2), (7, 0), (6, 0), (4, 1), (4, 3), (5, 3), (7, 3),
    (6, 1), (7, 2), (5, 1), (6, 3), (4, 2), (7, 1), (5, 2), (6, 2),
)
MULTIPLY_AT = 24
RELAY_AT = (13, 19)


def early_blocks(yh):
    return ((yh * 5, yh * 5 + 1), (yh * 5 + 2, yh * 5 + 3), (10 + yh, 12 + yh))


def late_blocks(yh):
    o = 1 - yh
    return (
        (yh * 5 + 4, o * 5), (o * 5 + 1, o * 5 + 2), (o * 5 + 3, o * 5 + 4), (10 + o, 12 + o),
    )


def block(b):
    return pl.ds(pl.multiple_of(b * COLS, COLS), COLS)


def pair_product(t, w, rows, pair):
    both = jnp.concatenate([w[block(pair[0]), :], w[block(pair[1]), :]], 0)
    return lax.dot_general(
        t[rows, :], both, (((1,), (1,)), ((), ())), preferred_element_type=jnp.float32
    ).astype(jnp.bfloat16)


def gather_kernel(shape, shard, toks, w, t4, acc, wsend, wrecv, psend, tsend, trecv, loc):
    qr, kr = shape
    n = qr + 2 * kr
    qn, kn = 32 * qr, 32 * kr
    cut = qr // SUB // 2 * SUB + SUB
    rep, tp = lax.axis_index("rep"), lax.axis_index("tp")
    x, yh, z = rep // 8, (rep // 4) % 2, rep % 4
    thi, tlo = tp // 2, tp % 2

    def at(x_, yh_, z_):
        return x_ * 8 + yh_ * 4 + z_

    x1 = x + 1 - 2 * (x % 2)
    x3 = 3 - x
    role0 = x == tp
    role3 = x == 3 - tp
    flip = at(x, 1 - yh, z)
    zp, zm = at(x, yh, (z + 1) % 4), at(x, yh, (z + 3) % 4)
    px1, px3 = at(x1, yh, z), at(x3, yh, z)

    barrier = pltpu.get_barrier_semaphore()
    peers = [(rep, (tp + k) % 4) for k in (1, 2, 3)]
    peers += [(flip, (tp + k) % 4) for k in range(4)]
    peers += [(p, tp) for p in (zp, zm, px1, px3)]
    for peer in peers:
        pl.semaphore_signal(barrier, inc=1, device_id=peer, device_id_type=MESH)
    pl.semaphore_wait(barrier, len(peers))

    def spans(j, part):
        if part == 0:
            return ((j * qr, cut),)
        return ((j * qr + cut, qr - cut), (qn + j * kr, kr), (qn + kn + j * kr, kr))

    def own_spans(part):
        if part == 0:
            return ((0, cut),)
        return ((cut, qr - cut), (qr, kr), (qr + kr, kr))

    def cut_of(ref, span):
        return ref.at[pl.ds(pl.multiple_of(span[0], SUB), span[1])]

    def settle(part, sem):
        size = cut if part == 0 else n - cut
        pltpu.make_async_copy(w.at[pl.ds(0, size)], w.at[pl.ds(0, size)], sem).wait()

    def send(src, src_spans, j, part, src_sem, dev):
        for s, d in zip(src_spans, spans(j, part)):
            pltpu.make_async_remote_copy(
                src_ref=cut_of(src, s), dst_ref=cut_of(w, d), send_sem=src_sem,
                recv_sem=wrecv.at[j * 2 + part], device_id=dev, device_id_type=MESH,
            ).start()

    me = (yh * 4 + z) * 4 + tp
    for part in range(2):
        @pl.when(role0)
        def _(part=part):
            for s, d in zip(own_spans(part), spans(me, part)):
                pltpu.make_async_copy(cut_of(shard, s), cut_of(w, d), wrecv.at[me * 2 + part]).start()

        @pl.when(jnp.logical_not(role0))
        def _(part=part):
            send(shard, own_spans(part), me, part, psend.at[0, part], (rep, x))

    crosses = jnp.logical_and(thi == x // 2, tlo != x % 2)
    for part in range(2):
        @pl.when(jnp.logical_not(crosses))
        def _(part=part):
            send(shard, own_spans(part), me, part, psend.at[1, part], (flip, x))

    rows = toks.shape[0]
    pieces = len(RELAY_AT)
    size = rows // pieces
    sib = thi * 2 + (1 - tlo)
    far = (1 - thi) * 2 + tlo
    fars = (1 - thi) * 2 + (1 - tlo)
    own = pltpu.make_async_copy(toks, t4.at[pl.ds(pl.multiple_of(tp * rows, rows), rows)], loc)
    own.start()

    def slot(r, part):
        return t4.at[pl.ds(pl.multiple_of(r * rows + part * size, size), size)]

    def tok(src, r, part, sem, dev):
        return pltpu.make_async_remote_copy(
            src_ref=src, dst_ref=slot(r, part), send_sem=tsend.at[sem, part],
            recv_sem=trecv.at[r, part], device_id=(rep, dev), device_id_type=MESH,
        )

    for kind, dev in ((0, far), (1, sib)):
        for part in range(pieces):
            tok(toks.at[pl.ds(part * size, size)], tp, part, kind, dev).start()

    def token_wait(r, part):
        pltpu.make_async_copy(slot(r, part), slot(r, part), trecv.at[r, part]).wait()

    def shard_of(i, d):
        h, m, c = i // 4, (i // 2) % 2, i % 2
        zs = (z + d) % 4
        tq = ((thi + m + h) % 2) * 2 + (tlo + c) % 2
        return (((yh + h) % 2) * 4 + zs) * 4 + tq

    def sends_of(i, d):
        kind = CLASSES[i]
        upward = (HALF[i] + tlo) % 2 == 0
        out = []
        if kind != "c":
            only = None if kind == "B" else role0
            if d in (0, 3):
                out.append((zp, only if d == 0 else upward if only is None else jnp.logical_and(only, upward)))
            if d in (0, 1):
                down = jnp.logical_not(upward)
                out.append((zm, only if d == 0 else down if only is None else jnp.logical_and(only, down)))
        if kind == "C":
            out.append((flip, role0))
        if kind != "B" or d == 0:
            out.append((px1, jnp.logical_or(role0, role3)))
            out.append((px3, role0))
        return out

    def guarded(cond, fn):
        if cond is None:
            fn()
        else:
            pl.when(cond)(fn)

    issued = []

    def multiply(piece):
        pair = early_blocks(yh)[piece // 2]
        half = t4.shape[0] // 2
        at_rows = pl.ds(piece % 2 * half, half)
        got = pair_product(t4, w, at_rows, pair)
        for k in range(2):
            acc[at_rows, block(pair[k])] = got[:, k * COLS : (k + 1) * COLS]

    for step, (i, d) in enumerate(ORDER):
        if step == MULTIPLY_AT:
            own.wait()
            for r in (sib, fars):
                for part in range(pieces):
                    token_wait(r, part)
        if MULTIPLY_AT <= step < MULTIPLY_AT + 6:
            multiply(step - MULTIPLY_AT)
        j = shard_of(i, d)
        for part in range(2):
            settle(part, wrecv.at[j * 2 + part])
            for dev, cond in sends_of(i, d):
                sem = wsend.at[len(issued)]
                guarded(cond, lambda dev=dev, sem=sem, part=part: send(w, spans(j, part), j, part, sem, (dev, tp)))
                issued.append((part, cond, sem))
        for part, when in enumerate(RELAY_AT):
            if step == when:
                token_wait(far, part)
                tok(slot(far, part), far, part, 2, sib).start()

    for kind in range(3):
        for part in range(pieces):
            pltpu.make_async_copy(slot(0, 0), slot(0, 0), tsend.at[kind, part]).wait()
    for part in range(2):
        guarded(jnp.logical_not(role0), lambda part=part: settle(part, psend.at[0, part]))
        guarded(jnp.logical_not(crosses), lambda part=part: settle(part, psend.at[1, part]))
    for part, cond, sem in issued:
        guarded(cond, lambda part=part, sem=sem: settle(part, sem))


def send_count():
    count = 0
    for kind in CLASSES:
        count += {"B": 4 + 2 + 2 * 0, "A": 4 + 2 + 6, "C": 4 + 2 + 6 + 4, "c": 8}[kind]
    return 2 * count


def product_kernel(w, t, acc, w_out, p_out, rest, wsem, psem):
    keep = pltpu.make_async_copy(w, w_out, wsem)
    keep.start()
    yh = (lax.axis_index("rep") // 4) % 2
    puts = []

    def put(src, b):
        puts.append(pltpu.make_async_copy(src, p_out.at[:, block(b)], psem.at[len(puts)]))
        puts[-1].start()

    for pair in early_blocks(yh):
        for b in pair:
            put(acc.at[:, block(b)], b)
    for k, pair in enumerate(late_blocks(yh)):
        rest[k] = pair_product(t, w, slice(None), pair)
        for m in range(2):
            put(rest.at[k, :, pl.ds(m * COLS, COLS)], pair[m])
    for p in puts:
        p.wait()
    keep.wait()


def shards(q_weight, key_projection_weight, value_projection_weight, tokens):
    width = q_weight.shape[1]
    qr, kr = q_weight.shape[0], key_projection_weight.shape[0]
    rows = 32 * (qr + 2 * kr)
    count = 4 * tokens.shape[0]
    shard = jnp.concatenate(
        [q_weight, key_projection_weight, value_projection_weight], 0
    ).astype(jnp.bfloat16)
    inside = [
        pltpu.VMEM((rows, width), jnp.bfloat16),
        pltpu.VMEM((count, width), jnp.bfloat16),
        pltpu.VMEM((count, rows), jnp.bfloat16),
    ]
    held = pl.pallas_call(
        functools.partial(gather_kernel, (qr, kr)),
        out_shape=inside,
        in_specs=[
            pl.BlockSpec(memory_space=pltpu.VMEM),
            pl.BlockSpec(memory_space=pl.ANY),
        ],
        out_specs=[pl.BlockSpec(memory_space=pltpu.VMEM)] * 3,
        scratch_shapes=[
            pltpu.SemaphoreType.DMA((send_count(),)),
            pltpu.SemaphoreType.DMA((64,)),
            pltpu.SemaphoreType.DMA((2, 2)),
            pltpu.SemaphoreType.DMA((3, len(RELAY_AT))),
            pltpu.SemaphoreType.DMA((4, len(RELAY_AT))),
            pltpu.SemaphoreType.DMA,
        ],
        compiler_params=pltpu.CompilerParams(
            has_side_effects=True, collective_id=0, vmem_limit_bytes=12 << 20
        ),
        name="gather",
    )(shard, pltpu.with_memory_space_constraint(tokens, pltpu.HBM))
    return pl.pallas_call(
        product_kernel,
        out_shape=(
            jax.ShapeDtypeStruct((rows, width), jnp.bfloat16),
            jax.ShapeDtypeStruct((count, rows), jnp.bfloat16),
        ),
        in_specs=[pl.BlockSpec(memory_space=pltpu.VMEM)] * 3,
        out_specs=(pl.BlockSpec(memory_space=pltpu.HBM),) * 2,
        scratch_shapes=[
            pltpu.VMEM((4, count, 2 * COLS), jnp.bfloat16),
            pltpu.SemaphoreType.DMA,
            pltpu.SemaphoreType.DMA((14,)),
        ],
        compiler_params=pltpu.CompilerParams(vmem_limit_bytes=8 << 20),
        name="product",
    )(*(pltpu.with_memory_space_constraint(a, pltpu.VMEM) for a in held))


def solution(mesh):
    both = P(("rep", "tp"), None)
    return jax.shard_map(
        shards, mesh=mesh, in_specs=(both,) * 4, out_specs=(P("tp", None), P("rep", "tp")),
        check_vma=False,
    )
```

```python
import functools

import jax
import jax.numpy as jnp
from jax import lax
from jax.experimental import pallas as pl
from jax.experimental.pallas import tpu as pltpu
from jax.sharding import PartitionSpec as P

MESH = pl.DeviceIdType.MESH
SUB = 8
COLS = 128

CLASSES = "BCBMBBBc"
HALF = (1, 0, 1, 1, 0, 0, 0, 0)
ORDER = (
    (
        0, 4, 12, 1, 16, 13, 8, 15, 20, 24, 7, 5, 9, 23, 3, 28,
        14, 11, 31, 6, 25, 29, 21, 30, 10, 27, 2, 17, 19, 22, 26, 18,
    ),
    (
        0, 16, 13, 8, 12, 15, 1, 9, 20, 3, 11, 14, 24, 28, 4, 7,
        10, 17, 23, 2, 6, 21, 5, 31, 25, 27, 29, 19, 22, 26, 30, 18,
    ),
    (
        0, 3, 4, 16, 8, 9, 15, 13, 20, 7, 1, 5, 24, 21, 12, 17,
        23, 19, 11, 14, 2, 27, 25, 28, 6, 31, 10, 18, 29, 26, 22, 30,
    ),
    (
        0, 3, 4, 1, 12, 16, 15, 13, 8, 20, 7, 24, 5, 23, 14, 28,
        2, 19, 31, 9, 17, 11, 25, 6, 29, 27, 10, 21, 18, 30, 22, 26,
    ),
)
MULTIPLY_AT = 27
RELAY_AT = (11, 23)
PIECES = 12
MULTIPLY_PARTS = (0, 1)


def early_blocks(yh):
    return ((yh * 5, yh * 5 + 1), (yh * 5 + 2, yh * 5 + 3), (10 + yh, 12 + yh))


def late_blocks(yh, k):
    o = 1 - yh
    first = jnp.where(k == 0, yh * 5 + 4, jnp.where(k == 3, 10 + o, o * 5 + 2 * k - 1))
    return first, jnp.where(k == 3, 12 + o, o * 5 + 2 * k)


def block(b):
    return pl.ds(pl.multiple_of(b * COLS, COLS), COLS)


def pair_product(t, w, rows, pair):
    both = jnp.concatenate([w[block(pair[0]), :], w[block(pair[1]), :]], 0)
    return lax.dot_general(
        t[rows, :], both, (((1,), (1,)), ((), ())), preferred_element_type=jnp.float32
    ).astype(jnp.bfloat16)


def gather_kernel(shape, shard, toks, w, t4, acc, wsend, wrecv, psend, tsend, trecv, loc):
    qr, kr = shape
    n = qr + 2 * kr
    qn, kn = 32 * qr, 32 * kr
    cut = qr // SUB // 2 * SUB + SUB
    rep, tp = lax.axis_index("rep"), lax.axis_index("tp")
    x, yh, z = rep // 8, (rep // 4) % 2, rep % 4
    thi, tlo = tp // 2, tp % 2

    def at(x_, yh_, z_):
        return x_ * 8 + yh_ * 4 + z_

    x1 = x + 1 - 2 * (x % 2)
    x3 = 3 - x
    role0 = x == tp
    flip = at(x, 1 - yh, z)
    zp, zm = at(x, yh, (z + 1) % 4), at(x, yh, (z + 3) % 4)
    px1, px3 = at(x1, yh, z), at(x3, yh, z)

    barrier = pltpu.get_barrier_semaphore()
    peers = [(rep, (tp + k) % 4) for k in (1, 2, 3)]
    peers += [(flip, (tp + k) % 4) for k in range(4)]
    peers += [(p, tp) for p in (zp, zm, px1, px3)]
    for peer in peers:
        pl.semaphore_signal(barrier, inc=1, device_id=peer, device_id_type=MESH)
    pl.semaphore_wait(barrier, len(peers))

    def spans(j, part):
        if part == 0:
            return ((j * qr, cut),)
        return ((j * qr + cut, qr - cut), (qn + j * kr, kr), (qn + kn + j * kr, kr))

    def own_spans(part):
        if part == 0:
            return ((0, cut),)
        return ((cut, qr - cut), (qr, kr), (qr + kr, kr))

    def cut_of(ref, span):
        return ref.at[pl.ds(pl.multiple_of(span[0], SUB), span[1])]

    def settle(part, sem):
        size = cut if part == 0 else n - cut
        pltpu.make_async_copy(w.at[pl.ds(0, size)], w.at[pl.ds(0, size)], sem).wait()

    def send(src, src_spans, j, part, src_sem, dev):
        for s, d in zip(src_spans, spans(j, part)):
            pltpu.make_async_remote_copy(
                src_ref=cut_of(src, s), dst_ref=cut_of(w, d), send_sem=src_sem,
                recv_sem=wrecv.at[j * 2 + part], device_id=dev, device_id_type=MESH,
            ).start()

    me = (yh * 4 + z) * 4 + tp
    for part in range(2):
        @pl.when(role0)
        def _(part=part):
            for s, d in zip(own_spans(part), spans(me, part)):
                pltpu.make_async_copy(cut_of(shard, s), cut_of(w, d), wrecv.at[me * 2 + part]).start()

        @pl.when(jnp.logical_not(role0))
        def _(part=part):
            send(shard, own_spans(part), me, part, psend.at[0, part], (rep, x))

    crosses = jnp.logical_and(thi == x // 2, tlo != x % 2)
    for part in range(2):
        @pl.when(jnp.logical_not(crosses))
        def _(part=part):
            send(shard, own_spans(part), me, part, psend.at[1, part], (flip, x))

    rows = toks.shape[0]
    pieces = len(RELAY_AT)
    size = rows // pieces
    sib = thi * 2 + (1 - tlo)
    far = (1 - thi) * 2 + tlo
    fars = (1 - thi) * 2 + (1 - tlo)
    own = pltpu.make_async_copy(toks, t4.at[pl.ds(pl.multiple_of(tp * rows, rows), rows)], loc)
    own.start()

    def slot(r, part):
        return t4.at[pl.ds(pl.multiple_of(r * rows + part * size, size), size)]

    def tok(src, r, part, sem, dev):
        return pltpu.make_async_remote_copy(
            src_ref=src, dst_ref=slot(r, part), send_sem=tsend.at[sem, part],
            recv_sem=trecv.at[r, part], device_id=(rep, dev), device_id_type=MESH,
        )

    for kind, dev in ((0, far), (1, sib)):
        for part in range(pieces):
            tok(toks.at[pl.ds(part * size, size)], tp, part, kind, dev).start()

    def token_wait(r, part):
        pltpu.make_async_copy(slot(r, part), slot(r, part), trecv.at[r, part]).wait()

    def shard_of(i, d):
        h, m, c = i // 4, (i // 2) % 2, i % 2
        zs = (z + d) % 4
        tq = ((thi + m + h) % 2) * 2 + (tlo + c) % 2
        return (((yh + h) % 2) * 4 + zs) * 4 + tq

    def sends_of(role, i, d):
        kind = CLASSES[i]
        upward = (HALF[i] + tlo) % 2 == 0
        out = []
        if kind == "B" or (role == 0 and kind in "AMC") or (role == 3 and kind == "M"):
            if d in (0, 3):
                out.append((zp, None if d == 0 else upward))
            if d in (0, 1):
                out.append((zm, None if d == 0 else jnp.logical_not(upward)))
        if kind == "C" and role == 0:
            out.append((flip, None))
        if role in (0, 3) and (kind != "B" or d == 0):
            out.append((px1, None))
        if role == 0 and (kind in "ACc" or d == 0):
            out.append((px3, None))
        return out

    def guarded(cond, fn):
        if cond is None:
            fn()
        else:
            pl.when(cond)(fn)

    role = (x % 2 + tlo) % 2 + 2 * ((x // 2 + thi) % 2)
    issued = [[], [], [], []]
    lines = t4.shape[0] // (PIECES // 3)

    def multiply(piece):
        pair = early_blocks(yh)[piece % 3]
        at_rows = pl.ds(piece // 3 * lines, lines)
        got = pair_product(t4, w, at_rows, pair)
        for k in range(2):
            acc[at_rows, block(pair[k])] = got[:, k * COLS : (k + 1) * COLS]

    def forward(k, step, part):
        i, d = divmod(ORDER[k][step], 4)
        j = shard_of(i, d)
        settle(part, wrecv.at[j * 2 + part])
        for n, (dev, cond) in enumerate(sends_of(k, i, d)):
            sem = wsend.at[len(issued[k])]
            guarded(cond, lambda dev=dev, sem=sem: send(w, spans(j, part), j, part, sem, (dev, tp)))
            issued[k].append((part, i, d, n))

    done = 0
    for step in range(32):
        if step == MULTIPLY_AT:
            own.wait()
            for r in (sib, fars):
                for part in range(pieces):
                    token_wait(r, part)
        for part in range(2):
            if step >= MULTIPLY_AT and done < PIECES and part in MULTIPLY_PARTS:
                multiply(done)
                done += 1
            for k in range(4):
                pl.when(role == k)(lambda k=k, part=part: forward(k, step, part))
        for part, when in enumerate(RELAY_AT):
            if step == when:
                token_wait(far, part)
                tok(slot(far, part), far, part, 2, sib).start()
    for piece in range(done, PIECES):
        multiply(piece)

    for kind in range(3):
        for part in range(pieces):
            pltpu.make_async_copy(slot(0, 0), slot(0, 0), tsend.at[kind, part]).wait()
    for part in range(2):
        guarded(jnp.logical_not(role0), lambda part=part: settle(part, psend.at[0, part]))
        guarded(jnp.logical_not(crosses), lambda part=part: settle(part, psend.at[1, part]))

    def drain(k):
        for at_sem, (part, i, d, n) in enumerate(issued[k]):
            cond = sends_of(k, i, d)[n][1]
            guarded(cond, lambda at_sem=at_sem, part=part: settle(part, wsend.at[at_sem]))

    for k in range(4):
        pl.when(role == k)(lambda k=k: drain(k))


def send_count():
    return 2 * sum({"B": 6, "A": 12, "M": 9, "C": 16, "c": 8}[kind] for kind in CLASSES)


def product_kernel(w, t, acc, w_out, p_out, rest, wsem, psem):
    keep = pltpu.make_async_copy(w, w_out, wsem)
    keep.start()
    yh = (lax.axis_index("rep") // 4) % 2

    def put(src, b, sem):
        return pltpu.make_async_copy(src, p_out.at[:, block(b)], sem)

    early = [b for pair in early_blocks(yh) for b in pair]
    early = [put(acc.at[:, block(b)], b, psem.at[8 + n]) for n, b in enumerate(early)]
    for p in early:
        p.start()

    def late(k):
        pair = late_blocks(yh, k)
        return [put(rest.at[k, :, pl.ds(m * COLS, COLS)], pair[m], psem.at[2 * k + m]) for m in range(2)]

    def step(k, carry):
        rest[k] = pair_product(t, w, slice(None), late_blocks(yh, k))
        for p in late(k):
            p.start()
        return carry

    lax.fori_loop(0, 4, step, 0)

    def finish(k, carry):
        for p in late(k):
            p.wait()
        return carry

    lax.fori_loop(0, 4, finish, 0)
    for p in early:
        p.wait()
    keep.wait()


def cast_kernel(q, k, v, out):
    at = 0
    for part in (q, k, v):
        out[pl.ds(at, part.shape[0]), :] = part[...].astype(jnp.bfloat16)
        at += part.shape[0]


def shards(q_weight, key_projection_weight, value_projection_weight, tokens):
    width = q_weight.shape[1]
    qr, kr = q_weight.shape[0], key_projection_weight.shape[0]
    rows = 32 * (qr + 2 * kr)
    count = 4 * tokens.shape[0]
    shard = pl.pallas_call(
        cast_kernel,
        out_shape=pltpu.VMEM((qr + 2 * kr, width), jnp.bfloat16),
        in_specs=[pl.BlockSpec(memory_space=pltpu.VMEM)] * 3,
        out_specs=pl.BlockSpec(memory_space=pltpu.VMEM),
        compiler_params=pltpu.CompilerParams(vmem_limit_bytes=4 << 20),
        name="cast",
    )(q_weight, key_projection_weight, value_projection_weight)
    inside = [
        pltpu.VMEM((rows, width), jnp.bfloat16),
        pltpu.VMEM((count, width), jnp.bfloat16),
        pltpu.VMEM((count, rows), jnp.bfloat16),
    ]
    held = pl.pallas_call(
        functools.partial(gather_kernel, (qr, kr)),
        out_shape=inside,
        in_specs=[
            pl.BlockSpec(memory_space=pltpu.VMEM),
            pl.BlockSpec(memory_space=pl.ANY),
        ],
        out_specs=[pl.BlockSpec(memory_space=pltpu.VMEM)] * 3,
        scratch_shapes=[
            pltpu.SemaphoreType.DMA((send_count(),)),
            pltpu.SemaphoreType.DMA((64,)),
            pltpu.SemaphoreType.DMA((2, 2)),
            pltpu.SemaphoreType.DMA((3, len(RELAY_AT))),
            pltpu.SemaphoreType.DMA((4, len(RELAY_AT))),
            pltpu.SemaphoreType.DMA,
        ],
        compiler_params=pltpu.CompilerParams(
            has_side_effects=True, collective_id=0, vmem_limit_bytes=12 << 20
        ),
        name="gather",
    )(
        pltpu.with_memory_space_constraint(shard, pltpu.VMEM),
        pltpu.with_memory_space_constraint(tokens, pltpu.HBM),
    )
    return pl.pallas_call(
        product_kernel,
        out_shape=(
            jax.ShapeDtypeStruct((rows, width), jnp.bfloat16),
            jax.ShapeDtypeStruct((count, rows), jnp.bfloat16),
        ),
        in_specs=[pl.BlockSpec(memory_space=pltpu.VMEM)] * 3,
        out_specs=(pl.BlockSpec(memory_space=pltpu.HBM),) * 2,
        scratch_shapes=[
            pltpu.VMEM((4, count, 2 * COLS), jnp.bfloat16),
            pltpu.SemaphoreType.DMA,
            pltpu.SemaphoreType.DMA((14,)),
        ],
        compiler_params=pltpu.CompilerParams(vmem_limit_bytes=8 << 20),
        name="product",
    )(*(pltpu.with_memory_space_constraint(a, pltpu.VMEM) for a in held))


def solution(mesh):
    both = P(("rep", "tp"), None)
    return jax.shard_map(
        shards, mesh=mesh, in_specs=(both,) * 4, out_specs=(P("tp", None), P("rep", "tp")),
        check_vma=False,
    )
```

```python
import functools

import jax
import jax.numpy as jnp
from jax import lax
from jax.experimental import pallas as pl
from jax.experimental.pallas import tpu as pltpu
from jax.sharding import PartitionSpec as P

MESH = pl.DeviceIdType.MESH
SUB = 8
COLS = 128

CLASSES = ("MBMMMBBA", "MCBBBBBc")
TREES = ("qkqqwqww", "qqkwkqqq")
HALF = ((0, 1, 0, 1, 1, 0, 1, 1), (0, 1, 0, 1, 0, 1, 0, 0))
ORDER = (
    (
        0, 1, 6, 8, 24, 9, 25, 30, 7, 14, 16, 17, 15, 10, 2, 11, 3, 18, 5, 33, 26, 40,
        4, 22, 56, 32, 23, 48, 20, 27, 49, 13, 35, 12, 46, 58, 62, 19, 41, 39, 50, 42, 34, 31,
        29, 21, 59, 28, 38, 63, 47, 51, 36, 43, 55, 57, 60, 61, 54, 37, 44, 53, 45, 52,
    ),
    (
        0, 8, 5, 3, 25, 31, 30, 4, 56, 40, 6, 16, 26, 9, 27, 24, 15, 14, 17, 20, 42, 11,
        13, 22, 7, 2, 29, 1, 48, 10, 49, 19, 46, 62, 18, 23, 41, 58, 38, 54, 44, 32, 34, 33,
        50, 28, 21, 12, 51, 35, 55, 57, 47, 39, 36, 60, 43, 59, 63, 52, 53, 61, 37, 45,
    ),
    (
        0, 1, 6, 3, 8, 17, 25, 9, 56, 22, 26, 31, 15, 11, 27, 14, 23, 18, 10, 30, 40, 13,
        19, 2, 29, 12, 48, 32, 4, 7, 16, 33, 21, 42, 24, 54, 28, 46, 50, 20, 49, 41, 62, 5,
        35, 38, 39, 34, 52, 55, 51, 36, 58, 43, 47, 63, 57, 37, 59, 44, 60, 53, 61, 45,
    ),
    (
        0, 2, 8, 24, 1, 3, 7, 6, 30, 17, 15, 4, 16, 23, 22, 18, 10, 25, 32, 14, 26, 5,
        9, 48, 19, 31, 27, 11, 40, 13, 33, 56, 12, 46, 28, 21, 29, 50, 20, 34, 49, 38, 39, 42,
        54, 44, 41, 62, 36, 58, 43, 55, 59, 51, 35, 63, 52, 57, 47, 61, 60, 53, 45, 37,
    ),
)
MULTIPLY_AT = (48, 49, 49, 52, 55, 59)
RELAY_AT = (31, 32)


def early_blocks(yh):
    return ((yh * 5, yh * 5 + 1), (yh * 5 + 2, yh * 5 + 3), (10 + yh, 12 + yh))


def late_blocks(yh, k):
    o = 1 - yh
    first = jnp.where(k == 0, yh * 5 + 4, jnp.where(k == 3, 10 + o, o * 5 + 2 * k - 1))
    return first, jnp.where(k == 3, 12 + o, o * 5 + 2 * k)


def block(b):
    return pl.ds(pl.multiple_of(b * COLS, COLS), COLS)


def pair_product(t, w, rows, pair):
    both = jnp.concatenate([w[block(pair[0]), :], w[block(pair[1]), :]], 0)
    return lax.dot_general(
        t[rows, :], both, (((1,), (1,)), ((), ())), preferred_element_type=jnp.float32
    ).astype(jnp.bfloat16)


def gather_kernel(shape, shard, toks, w, t4, acc, wsend, wrecv, psend, tsend, trecv, loc):
    qr, kr = shape
    n = qr + 2 * kr
    qn, kn = 32 * qr, 32 * kr
    cut = qr // SUB // 2 * SUB + SUB
    rep, tp = lax.axis_index("rep"), lax.axis_index("tp")
    x, yh, z = rep // 8, (rep // 4) % 2, rep % 4
    thi, tlo = tp // 2, tp % 2

    def at(x_, yh_, z_):
        return x_ * 8 + yh_ * 4 + z_

    x1 = x + 1 - 2 * (x % 2)
    x3 = 3 - x
    role0 = x == tp
    flip = at(x, 1 - yh, z)
    zp, zm = at(x, yh, (z + 1) % 4), at(x, yh, (z + 3) % 4)
    px1, px3 = at(x1, yh, z), at(x3, yh, z)

    barrier = pltpu.get_barrier_semaphore()
    peers = [(rep, (tp + k) % 4) for k in (1, 2, 3)]
    peers += [(flip, (tp + k) % 4) for k in range(4)]
    peers += [(p, tp) for p in (zp, zm, px1, px3)]
    for peer in peers:
        pl.semaphore_signal(barrier, inc=1, device_id=peer, device_id_type=MESH)
    pl.semaphore_wait(barrier, len(peers))

    def spans(j, part):
        if part == 0:
            return ((j * qr, cut),)
        return ((j * qr + cut, qr - cut), (qn + j * kr, kr), (qn + kn + j * kr, kr))

    def own_spans(part):
        if part == 0:
            return ((0, cut),)
        return ((cut, qr - cut), (qr, kr), (qr + kr, kr))

    def cut_of(ref, span):
        return ref.at[pl.ds(pl.multiple_of(span[0], SUB), span[1])]

    def settle(part, sem):
        size = cut if part == 0 else n - cut
        pltpu.make_async_copy(w.at[pl.ds(0, size)], w.at[pl.ds(0, size)], sem).wait()

    def send(src, src_spans, j, part, src_sem, dev):
        for s, d in zip(src_spans, spans(j, part)):
            pltpu.make_async_remote_copy(
                src_ref=cut_of(src, s), dst_ref=cut_of(w, d), send_sem=src_sem,
                recv_sem=wrecv.at[j * 2 + part], device_id=dev, device_id_type=MESH,
            ).start()

    me = (yh * 4 + z) * 4 + tp
    for part in range(2):
        @pl.when(role0)
        def _(part=part):
            for s, d in zip(own_spans(part), spans(me, part)):
                pltpu.make_async_copy(cut_of(shard, s), cut_of(w, d), wrecv.at[me * 2 + part]).start()

        @pl.when(jnp.logical_not(role0))
        def _(part=part):
            send(shard, own_spans(part), me, part, psend.at[0, part], (rep, x))

    seen = 4 + 2 * (1 - (thi + x // 2) % 2) + (tlo + x) % 2

    def goes_early(part):
        keep = jnp.bool_(True)
        for i in range(4, 8):
            if CLASSES[part][i] == "c":
                keep = jnp.logical_and(keep, seen != i)
        return keep

    for part in range(2):
        @pl.when(goes_early(part))
        def _(part=part):
            send(shard, own_spans(part), me, part, psend.at[1, part], (flip, x))

    rows = toks.shape[0]
    pieces = len(RELAY_AT)
    size = rows // pieces
    sib = thi * 2 + (1 - tlo)
    far = (1 - thi) * 2 + tlo
    fars = (1 - thi) * 2 + (1 - tlo)
    own = pltpu.make_async_copy(toks, t4.at[pl.ds(pl.multiple_of(tp * rows, rows), rows)], loc)
    own.start()

    def slot(r, part):
        return t4.at[pl.ds(pl.multiple_of(r * rows + part * size, size), size)]

    def tok(src, r, part, sem, dev):
        return pltpu.make_async_remote_copy(
            src_ref=src, dst_ref=slot(r, part), send_sem=tsend.at[sem, part],
            recv_sem=trecv.at[r, part], device_id=(rep, dev), device_id_type=MESH,
        )

    for kind, dev in ((0, far), (1, sib)):
        for part in range(pieces):
            tok(toks.at[pl.ds(part * size, size)], tp, part, kind, dev).start()

    def token_wait(r, part):
        pltpu.make_async_copy(slot(r, part), slot(r, part), trecv.at[r, part]).wait()

    def shard_of(i, d):
        h, m, c = i // 4, (i // 2) % 2, i % 2
        zs = (z + d) % 4
        tq = ((thi + m + h) % 2) * 2 + (tlo + c) % 2
        return (((yh + h) % 2) * 4 + zs) * 4 + tq

    def sends_of(role, i, d, part):
        kind, tree = CLASSES[part][i], TREES[part][i]
        upward = (HALF[part][i] + tlo) % 2 == 0
        out = []
        if kind == "B" or (role == 0 and kind in "AMC") or (role == 3 and kind == "M"):
            if d in (0, 3):
                out.append((zp, None if d == 0 else upward))
            if d in (0, 1):
                out.append((zm, None if d == 0 else jnp.logical_not(upward)))
        if kind == "C" and role == 0:
            out.append((flip, None))
        if kind == "M":
            near, over = role in (0, 3), role == 0 and d == 0
        elif kind == "B" and d != 0:
            near, over = False, False
        else:
            near = role in {"q": (0, 3), "w": (0,), "k": (3,)}[tree]
            over = role in {"q": (0,), "w": (0, 1), "k": (0, 2)}[tree]
        if near:
            out.append((px1, None))
        if over:
            out.append((px3, None))
        return out

    def guarded(cond, fn):
        if cond is None:
            fn()
        else:
            pl.when(cond)(fn)

    role = (x % 2 + tlo) % 2 + 2 * ((x // 2 + thi) % 2)
    issued = [[], [], [], []]
    lines = t4.shape[0] // (len(MULTIPLY_AT) // 3)

    def multiply(piece):
        if piece == 0:
            own.wait()
            for r in (sib, fars):
                for part in range(pieces):
                    token_wait(r, part)
        pair = early_blocks(yh)[piece % 3]
        at_rows = pl.ds(piece // 3 * lines, lines)
        got = pair_product(t4, w, at_rows, pair)
        for k in range(2):
            acc[at_rows, block(pair[k])] = got[:, k * COLS : (k + 1) * COLS]

    def forward(k, step):
        i, d, part = ORDER[k][step] // 8, ORDER[k][step] // 2 % 4, ORDER[k][step] % 2
        j = shard_of(i, d)
        settle(part, wrecv.at[j * 2 + part])
        for n, (dev, cond) in enumerate(sends_of(k, i, d, part)):
            sem = wsend.at[len(issued[k])]
            guarded(cond, lambda dev=dev, sem=sem: send(w, spans(j, part), j, part, sem, (dev, tp)))
            issued[k].append((part, i, d, n))

    for step in range(65):
        for piece, when in enumerate(MULTIPLY_AT):
            if step == when:
                multiply(piece)
        if step == 64:
            break
        for k in range(4):
            pl.when(role == k)(lambda k=k: forward(k, step))
        for part, when in enumerate(RELAY_AT):
            if step == when:
                token_wait(far, part)
                tok(slot(far, part), far, part, 2, sib).start()

    for kind in range(3):
        for part in range(pieces):
            pltpu.make_async_copy(slot(0, 0), slot(0, 0), tsend.at[kind, part]).wait()
    for part in range(2):
        guarded(jnp.logical_not(role0), lambda part=part: settle(part, psend.at[0, part]))
        guarded(goes_early(part), lambda part=part: settle(part, psend.at[1, part]))

    def drain(k):
        for at_sem, (part, i, d, n) in enumerate(issued[k]):
            cond = sends_of(k, i, d, part)[n][1]
            guarded(cond, lambda at_sem=at_sem, part=part: settle(part, wsend.at[at_sem]))

    for k in range(4):
        pl.when(role == k)(lambda k=k: drain(k))


def send_count():
    most = {"B": 6, "A": 12, "M": 9, "C": 16, "c": 8}
    return max(32, sum(most[kind] for line in CLASSES for kind in line))


def product_kernel(w, t, acc, w_out, p_out, rest, wsem, psem):
    keep = pltpu.make_async_copy(w, w_out, wsem)
    keep.start()
    yh = (lax.axis_index("rep") // 4) % 2

    def put(src, b, sem):
        return pltpu.make_async_copy(src, p_out.at[:, block(b)], sem)

    early = [b for pair in early_blocks(yh) for b in pair]
    early = [put(acc.at[:, block(b)], b, psem.at[8 + n]) for n, b in enumerate(early)]
    for p in early:
        p.start()

    def late(k):
        pair = late_blocks(yh, k)
        return [put(rest.at[k, :, pl.ds(m * COLS, COLS)], pair[m], psem.at[2 * k + m]) for m in range(2)]

    def step(k, carry):
        rest[k] = pair_product(t, w, slice(None), late_blocks(yh, k))
        for p in late(k):
            p.start()
        return carry

    lax.fori_loop(0, 4, step, 0)

    def finish(k, carry):
        for p in late(k):
            p.wait()
        return carry

    lax.fori_loop(0, 4, finish, 0)
    for p in early:
        p.wait()
    keep.wait()


def cast_kernel(q, k, v, out, wide, sems):
    at, parts = 0, []
    for n, part in enumerate((q, k, v)):
        rows = pl.ds(at, part.shape[0])
        parts.append((rows, pltpu.make_async_copy(part, wide.at[rows], sems.at[n])))
        parts[-1][1].start()
        at += part.shape[0]
    for rows, copy in parts:
        copy.wait()
        out[rows, :] = wide[rows, :].astype(jnp.bfloat16)


def shards(q_weight, key_projection_weight, value_projection_weight, tokens):
    width = q_weight.shape[1]
    qr, kr = q_weight.shape[0], key_projection_weight.shape[0]
    rows = 32 * (qr + 2 * kr)
    count = 4 * tokens.shape[0]
    shard = pl.pallas_call(
        cast_kernel,
        out_shape=pltpu.VMEM((qr + 2 * kr, width), jnp.bfloat16),
        in_specs=[pl.BlockSpec(memory_space=pltpu.HBM)] * 3,
        out_specs=pl.BlockSpec(memory_space=pltpu.VMEM),
        scratch_shapes=[
            pltpu.VMEM((qr + 2 * kr, width), jnp.float32),
            pltpu.SemaphoreType.DMA((3,)),
        ],
        compiler_params=pltpu.CompilerParams(vmem_limit_bytes=4 << 20),
        name="cast",
    )(*(
        pltpu.with_memory_space_constraint(a, pltpu.HBM)
        for a in (q_weight, key_projection_weight, value_projection_weight)
    ))
    inside = [
        pltpu.VMEM((rows, width), jnp.bfloat16),
        pltpu.VMEM((count, width), jnp.bfloat16),
        pltpu.VMEM((count, rows), jnp.bfloat16),
    ]
    held = pl.pallas_call(
        functools.partial(gather_kernel, (qr, kr)),
        out_shape=inside,
        in_specs=[
            pl.BlockSpec(memory_space=pltpu.VMEM),
            pl.BlockSpec(memory_space=pl.ANY),
        ],
        out_specs=[pl.BlockSpec(memory_space=pltpu.VMEM)] * 3,
        scratch_shapes=[
            pltpu.SemaphoreType.DMA((send_count(),)),
            pltpu.SemaphoreType.DMA((64,)),
            pltpu.SemaphoreType.DMA((2, 2)),
            pltpu.SemaphoreType.DMA((3, len(RELAY_AT))),
            pltpu.SemaphoreType.DMA((4, len(RELAY_AT))),
            pltpu.SemaphoreType.DMA,
        ],
        compiler_params=pltpu.CompilerParams(
            has_side_effects=True, collective_id=0, vmem_limit_bytes=12 << 20
        ),
        name="gather",
    )(
        pltpu.with_memory_space_constraint(shard, pltpu.VMEM),
        pltpu.with_memory_space_constraint(tokens, pltpu.HBM),
    )
    return pl.pallas_call(
        product_kernel,
        out_shape=(
            jax.ShapeDtypeStruct((rows, width), jnp.bfloat16),
            jax.ShapeDtypeStruct((count, rows), jnp.bfloat16),
        ),
        in_specs=[pl.BlockSpec(memory_space=pltpu.VMEM)] * 3,
        out_specs=(pl.BlockSpec(memory_space=pltpu.HBM),) * 2,
        scratch_shapes=[
            pltpu.VMEM((4, count, 2 * COLS), jnp.bfloat16),
            pltpu.SemaphoreType.DMA,
            pltpu.SemaphoreType.DMA((14,)),
        ],
        compiler_params=pltpu.CompilerParams(vmem_limit_bytes=8 << 20),
        name="product",
    )(*(pltpu.with_memory_space_constraint(a, pltpu.VMEM) for a in held))


def solution(mesh):
    both = P(("rep", "tp"), None)
    return jax.shard_map(
        shards, mesh=mesh, in_specs=(both,) * 4, out_specs=(P("tp", None), P("rep", "tp")),
        check_vma=False,
    )
```

```python
import functools

import jax
import jax.numpy as jnp
from jax import lax
from jax.experimental import pallas as pl
from jax.experimental.pallas import tpu as pltpu
from jax.sharding import PartitionSpec as P

MESH = pl.DeviceIdType.MESH
SUB = 8
COLS = 128

CLASSES = ("MBMMMBBA", "MCBBBBBc")
TREES = ("kkwqwwww", "qqkwkqqq")
HALF = ((1, 1, 0, 0, 1, 0, 1, 0), (0, 1, 0, 1, 0, 1, 1, 1))
ORDER = (
    (
        0, 1, 24, 2, 16, 9, 8, 17, 6, 7, 25, 23, 19, 3, 11, 14, 27, 40, 48, 32, 33, 10,
        30, 22, 5, 26, 56, 18, 15, 4, 31, 13, 49, 20, 62, 12, 41, 34, 21, 28, 58, 35, 59, 39,
        29, 51, 63, 55, 38, 50, 57, 42, 54, 60, 43, 53, 37, 61, 46, 47, 36, 44, 52, 45,
    ),
    (
        2, 0, 40, 16, 46, 25, 7, 22, 6, 27, 1, 8, 42, 9, 31, 32, 24, 17, 56, 5, 18, 10,
        4, 48, 30, 14, 13, 3, 15, 26, 49, 19, 23, 29, 20, 62, 41, 12, 21, 28, 51, 55, 33, 11,
        54, 58, 50, 63, 34, 43, 47, 57, 39, 59, 35, 60, 44, 52, 38, 53, 61, 45, 37, 36,
    ),
    (
        26, 1, 8, 30, 6, 16, 0, 17, 10, 19, 25, 23, 4, 27, 31, 2, 40, 11, 3, 14, 22, 9,
        32, 33, 5, 12, 48, 18, 28, 7, 21, 24, 42, 49, 13, 29, 62, 34, 39, 20, 50, 54, 41, 15,
        35, 55, 52, 56, 43, 51, 38, 46, 57, 47, 59, 44, 61, 45, 63, 58, 60, 36, 37, 53,
    ),
    (
        0, 1, 16, 24, 6, 30, 26, 2, 8, 22, 17, 3, 25, 40, 4, 7, 19, 32, 33, 48, 14, 5,
        11, 18, 31, 10, 28, 27, 46, 13, 54, 50, 23, 9, 21, 49, 12, 20, 29, 34, 38, 41, 47, 15,
        59, 42, 56, 63, 35, 57, 52, 62, 55, 51, 43, 39, 58, 36, 61, 37, 60, 53, 45, 44,
    ),
)
MULTIPLY_AT = (45, 46, 48, 48, 51, 55)
RELAY_AT = (28, 34)


def early_blocks(yh):
    return ((yh * 5, yh * 5 + 1), (yh * 5 + 2, yh * 5 + 3), (10 + yh, 12 + yh))


def late_blocks(yh, k):
    o = 1 - yh
    first = jnp.where(k == 0, yh * 5 + 4, jnp.where(k == 3, 10 + o, o * 5 + 2 * k - 1))
    return first, jnp.where(k == 3, 12 + o, o * 5 + 2 * k)


def block(b):
    return pl.ds(pl.multiple_of(b * COLS, COLS), COLS)


def pair_product(t, w, rows, pair):
    both = jnp.concatenate([w[block(pair[0]), :], w[block(pair[1]), :]], 0)
    return lax.dot_general(
        t[rows, :], both, (((1,), (1,)), ((), ())), preferred_element_type=jnp.float32
    ).astype(jnp.bfloat16)


def gather_kernel(shape, shard, toks, w, t4, acc, wsend, wrecv, psend, tsend, trecv, loc):
    qr, kr = shape
    n = qr + 2 * kr
    qn, kn = 32 * qr, 32 * kr
    cut = qr // SUB // 2 * SUB + SUB
    rep, tp = lax.axis_index("rep"), lax.axis_index("tp")
    x, yh, z = rep // 8, (rep // 4) % 2, rep % 4
    thi, tlo = tp // 2, tp % 2

    def at(x_, yh_, z_):
        return x_ * 8 + yh_ * 4 + z_

    x1 = x + 1 - 2 * (x % 2)
    x3 = 3 - x
    role0 = x == tp
    flip = at(x, 1 - yh, z)
    zp, zm = at(x, yh, (z + 1) % 4), at(x, yh, (z + 3) % 4)
    px1, px3 = at(x1, yh, z), at(x3, yh, z)

    barrier = pltpu.get_barrier_semaphore()
    peers = [(rep, (tp + k) % 4) for k in (1, 2, 3)]
    peers += [(flip, (tp + k) % 4) for k in range(4)]
    peers += [(p, tp) for p in (zp, zm, px1, px3)]
    for peer in peers:
        pl.semaphore_signal(barrier, inc=1, device_id=peer, device_id_type=MESH)
    pl.semaphore_wait(barrier, len(peers))

    def spans(j, part):
        if part == 0:
            return ((j * qr, cut),)
        return ((j * qr + cut, qr - cut), (qn + j * kr, kr), (qn + kn + j * kr, kr))

    def own_spans(part):
        if part == 0:
            return ((0, cut),)
        return ((cut, qr - cut), (qr, kr), (qr + kr, kr))

    def cut_of(ref, span):
        return ref.at[pl.ds(pl.multiple_of(span[0], SUB), span[1])]

    def settle(part, sem):
        size = cut if part == 0 else n - cut
        pltpu.make_async_copy(w.at[pl.ds(0, size)], w.at[pl.ds(0, size)], sem).wait()

    def send(src, src_spans, j, part, src_sem, dev):
        for s, d in zip(src_spans, spans(j, part)):
            pltpu.make_async_remote_copy(
                src_ref=cut_of(src, s), dst_ref=cut_of(w, d), send_sem=src_sem,
                recv_sem=wrecv.at[j * 2 + part], device_id=dev, device_id_type=MESH,
            ).start()

    me = (yh * 4 + z) * 4 + tp
    for part in range(2):
        @pl.when(role0)
        def _(part=part):
            for s, d in zip(own_spans(part), spans(me, part)):
                pltpu.make_async_copy(cut_of(shard, s), cut_of(w, d), wrecv.at[me * 2 + part]).start()

        @pl.when(jnp.logical_not(role0))
        def _(part=part):
            send(shard, own_spans(part), me, part, psend.at[0, part], (rep, x))

    seen = 4 + 2 * (1 - (thi + x // 2) % 2) + (tlo + x) % 2

    def goes_early(part):
        keep = jnp.bool_(True)
        for i in range(4, 8):
            if CLASSES[part][i] == "c":
                keep = jnp.logical_and(keep, seen != i)
        return keep

    for part in range(2):
        @pl.when(goes_early(part))
        def _(part=part):
            send(shard, own_spans(part), me, part, psend.at[1, part], (flip, x))

    rows = toks.shape[0]
    pieces = len(RELAY_AT)
    size = rows // pieces
    sib = thi * 2 + (1 - tlo)
    far = (1 - thi) * 2 + tlo
    fars = (1 - thi) * 2 + (1 - tlo)
    own = pltpu.make_async_copy(toks, t4.at[pl.ds(pl.multiple_of(tp * rows, rows), rows)], loc)
    own.start()

    def slot(r, part):
        return t4.at[pl.ds(pl.multiple_of(r * rows + part * size, size), size)]

    def tok(src, r, part, sem, dev):
        return pltpu.make_async_remote_copy(
            src_ref=src, dst_ref=slot(r, part), send_sem=tsend.at[sem, part],
            recv_sem=trecv.at[r, part], device_id=(rep, dev), device_id_type=MESH,
        )

    for kind, dev in ((0, far), (1, sib)):
        for part in range(pieces):
            tok(toks.at[pl.ds(part * size, size)], tp, part, kind, dev).start()

    def token_wait(r, part):
        pltpu.make_async_copy(slot(r, part), slot(r, part), trecv.at[r, part]).wait()

    def shard_of(i, d):
        h, m, c = i // 4, (i // 2) % 2, i % 2
        zs = (z + d) % 4
        tq = ((thi + m + h) % 2) * 2 + (tlo + c) % 2
        return (((yh + h) % 2) * 4 + zs) * 4 + tq

    def sends_of(role, i, d, part):
        kind, tree = CLASSES[part][i], TREES[part][i]
        upward = (HALF[part][i] + tlo) % 2 == 0
        out = []
        if kind == "B" or (role == 0 and kind in "AMC") or (role == 3 and kind == "M"):
            if d in (0, 3):
                out.append((zp, None if d == 0 else upward))
            if d in (0, 1):
                out.append((zm, None if d == 0 else jnp.logical_not(upward)))
        if kind == "C" and role == 0:
            out.append((flip, None))
        if kind == "M":
            near, over = role in (0, 3), role == 0 and d == 0
        elif kind == "B" and d != 0:
            near, over = False, False
        else:
            near = role in {"q": (0, 3), "w": (0,), "k": (3,)}[tree]
            over = role in {"q": (0,), "w": (0, 1), "k": (0, 2)}[tree]
        if near:
            out.append((px1, None))
        if over:
            out.append((px3, None))
        return out

    def guarded(cond, fn):
        if cond is None:
            fn()
        else:
            pl.when(cond)(fn)

    role = (x % 2 + tlo) % 2 + 2 * ((x // 2 + thi) % 2)
    issued = [[], [], [], []]
    lines = t4.shape[0] // (len(MULTIPLY_AT) // 3)

    def multiply(piece):
        if piece == 0:
            own.wait()
            for r in (sib, fars):
                for part in range(pieces):
                    token_wait(r, part)
        pair = early_blocks(yh)[piece % 3]
        at_rows = pl.ds(piece // 3 * lines, lines)
        got = pair_product(t4, w, at_rows, pair)
        for k in range(2):
            acc[at_rows, block(pair[k])] = got[:, k * COLS : (k + 1) * COLS]

    def forward(k, step):
        i, d, part = ORDER[k][step] // 8, ORDER[k][step] // 2 % 4, ORDER[k][step] % 2
        j = shard_of(i, d)
        settle(part, wrecv.at[j * 2 + part])
        for n, (dev, cond) in enumerate(sends_of(k, i, d, part)):
            sem = wsend.at[len(issued[k])]
            guarded(cond, lambda dev=dev, sem=sem: send(w, spans(j, part), j, part, sem, (dev, tp)))
            issued[k].append((part, i, d, n))

    for step in range(65):
        for piece, when in enumerate(MULTIPLY_AT):
            if step == when:
                multiply(piece)
        if step == 64:
            break
        for k in range(4):
            pl.when(role == k)(lambda k=k: forward(k, step))
        for part, when in enumerate(RELAY_AT):
            if step == when:
                token_wait(far, part)
                tok(slot(far, part), far, part, 2, sib).start()

    for kind in range(3):
        for part in range(pieces):
            pltpu.make_async_copy(slot(0, 0), slot(0, 0), tsend.at[kind, part]).wait()
    for part in range(2):
        guarded(jnp.logical_not(role0), lambda part=part: settle(part, psend.at[0, part]))
        guarded(goes_early(part), lambda part=part: settle(part, psend.at[1, part]))

    def drain(k):
        for at_sem, (part, i, d, n) in enumerate(issued[k]):
            cond = sends_of(k, i, d, part)[n][1]
            guarded(cond, lambda at_sem=at_sem, part=part: settle(part, wsend.at[at_sem]))

    for k in range(4):
        pl.when(role == k)(lambda k=k: drain(k))


def send_count():
    most = {"B": 6, "A": 12, "M": 9, "C": 16, "c": 8}
    return max(32, sum(most[kind] for line in CLASSES for kind in line))


def product_kernel(w, t, acc, w_out, p_out, rest, wsem, psem):
    keep = pltpu.make_async_copy(w, w_out, wsem)
    keep.start()
    yh = (lax.axis_index("rep") // 4) % 2

    def put(src, b, sem):
        return pltpu.make_async_copy(src, p_out.at[:, block(b)], sem)

    early = [b for pair in early_blocks(yh) for b in pair]
    early = [put(acc.at[:, block(b)], b, psem.at[8 + n]) for n, b in enumerate(early)]
    for p in early:
        p.start()

    def late(k):
        pair = late_blocks(yh, k)
        return [put(rest.at[k, :, pl.ds(m * COLS, COLS)], pair[m], psem.at[2 * k + m]) for m in range(2)]

    def step(k, carry):
        rest[k] = pair_product(t, w, slice(None), late_blocks(yh, k))
        for p in late(k):
            p.start()
        return carry

    lax.fori_loop(0, 4, step, 0)

    def finish(k, carry):
        for p in late(k):
            p.wait()
        return carry

    lax.fori_loop(0, 4, finish, 0)
    for p in early:
        p.wait()
    keep.wait()


def cast_kernel(q, k, v, out, wide, sems):
    at, parts = 0, []
    for n, part in enumerate((q, k, v)):
        rows = pl.ds(at, part.shape[0])
        parts.append((rows, pltpu.make_async_copy(part, wide.at[rows], sems.at[n])))
        parts[-1][1].start()
        at += part.shape[0]
    for rows, copy in parts:
        copy.wait()
        out[rows, :] = wide[rows, :].astype(jnp.bfloat16)


def shards(q_weight, key_projection_weight, value_projection_weight, tokens):
    width = q_weight.shape[1]
    qr, kr = q_weight.shape[0], key_projection_weight.shape[0]
    rows = 32 * (qr + 2 * kr)
    count = 4 * tokens.shape[0]
    shard = pl.pallas_call(
        cast_kernel,
        out_shape=pltpu.VMEM((qr + 2 * kr, width), jnp.bfloat16),
        in_specs=[pl.BlockSpec(memory_space=pltpu.HBM)] * 3,
        out_specs=pl.BlockSpec(memory_space=pltpu.VMEM),
        scratch_shapes=[
            pltpu.VMEM((qr + 2 * kr, width), jnp.float32),
            pltpu.SemaphoreType.DMA((3,)),
        ],
        compiler_params=pltpu.CompilerParams(vmem_limit_bytes=4 << 20),
        name="cast",
    )(*(
        pltpu.with_memory_space_constraint(a, pltpu.HBM)
        for a in (q_weight, key_projection_weight, value_projection_weight)
    ))
    inside = [
        pltpu.VMEM((rows, width), jnp.bfloat16),
        pltpu.VMEM((count, width), jnp.bfloat16),
        pltpu.VMEM((count, rows), jnp.bfloat16),
    ]
    held = pl.pallas_call(
        functools.partial(gather_kernel, (qr, kr)),
        out_shape=inside,
        in_specs=[
            pl.BlockSpec(memory_space=pltpu.VMEM),
            pl.BlockSpec(memory_space=pl.ANY),
        ],
        out_specs=[pl.BlockSpec(memory_space=pltpu.VMEM)] * 3,
        scratch_shapes=[
            pltpu.SemaphoreType.DMA((send_count(),)),
            pltpu.SemaphoreType.DMA((64,)),
            pltpu.SemaphoreType.DMA((2, 2)),
            pltpu.SemaphoreType.DMA((3, len(RELAY_AT))),
            pltpu.SemaphoreType.DMA((4, len(RELAY_AT))),
            pltpu.SemaphoreType.DMA,
        ],
        compiler_params=pltpu.CompilerParams(
            has_side_effects=True, collective_id=0, vmem_limit_bytes=12 << 20
        ),
        name="gather",
    )(
        pltpu.with_memory_space_constraint(shard, pltpu.VMEM),
        pltpu.with_memory_space_constraint(tokens, pltpu.HBM),
    )
    return pl.pallas_call(
        product_kernel,
        out_shape=(
            jax.ShapeDtypeStruct((rows, width), jnp.bfloat16),
            jax.ShapeDtypeStruct((count, rows), jnp.bfloat16),
        ),
        in_specs=[pl.BlockSpec(memory_space=pltpu.VMEM)] * 3,
        out_specs=(pl.BlockSpec(memory_space=pltpu.HBM),) * 2,
        scratch_shapes=[
            pltpu.VMEM((4, count, 2 * COLS), jnp.bfloat16),
            pltpu.SemaphoreType.DMA,
            pltpu.SemaphoreType.DMA((14,)),
        ],
        compiler_params=pltpu.CompilerParams(vmem_limit_bytes=8 << 20),
        name="product",
    )(*(pltpu.with_memory_space_constraint(a, pltpu.VMEM) for a in held))


def solution(mesh):
    both = P(("rep", "tp"), None)
    return jax.shard_map(
        shards, mesh=mesh, in_specs=(both,) * 4, out_specs=(P("tp", None), P("rep", "tp")),
        check_vma=False,
    )
```
